8 devices in a mesh: dp: 1 (over z), tp: 2 (over y), sp: 4 (over x, core).
Axes of the slice: x: 2, y: 2, z: 1, core: 2. Of those that a mesh axis runs over, the one named last changes fastest.
Arguments:
- hidden_in: bfloat16 [1, 4096, 4096], P('dp', 'sp')
- start_pos: int32 [1], P('dp')
- h_init: float32 [1, 2, 4096], P('dp', None, 'tp')
- k_cache: bfloat16 [1, 2048, 256], P('dp')
- v_cache: bfloat16 [1, 2048, 256], P('dp')
- w_x: bfloat16 [2, 4096, 4096], P(None, None, 'tp')
- w_y: bfloat16 [2, 4096, 4096], P(None, None, 'tp')
- conv_w: bfloat16 [2, 4, 4096], P(None, None, 'tp')
- conv_b: bfloat16 [2, 4096], P(None, 'tp')
- gate_wi: bfloat16 [2, 16, 256, 256], P(None, 'tp')
- gate_wa: bfloat16 [2, 16, 256, 256], P(None, 'tp')
- gate_bi: bfloat16 [2, 4096], P(None, 'tp')
- gate_ba: bfloat16 [2, 4096], P(None, 'tp')
- lru_lambda: float32 [2, 4096], P(None, 'tp')
- w_rnn_out: bfloat16 [2, 4096, 4096], P(None, 'tp')
- w_q: bfloat16 [4096, 4096], P(None, 'tp')
- w_k: bfloat16 [4096, 256], replicated
- w_v: bfloat16 [4096, 256], replicated
- w_attn_out: bfloat16 [4096, 4096], P('tp')
- w_gate: bfloat16 [3, 4096, 12288], P(None, None, 'tp')
- w_up: bfloat16 [3, 4096, 12288], P(None, None, 'tp')
- w_down: bfloat16 [3, 12288, 4096], P(None, 'tp')
Outputs:
- output 1: bfloat16 [1, 4096, 4096], P('dp', 'sp')
- output 2: float32 [1, 2, 4096], P('dp', None, 'tp')
- output 3: bfloat16 [1, 2, 3, 4096], P('dp', None, None, 'tp')
- output 4: bfloat16 [1, 2048, 256], P('dp')
- output 5: bfloat16 [1, 2048, 256], P('dp')
All inputs are finite; a program needn't handle non-finite values.
Results may differ from the reference program's by a relative error of at most 0.0186511.
Values are sent between devices in bfloat16 or wider.
A program may use at most 2.5 GiB of HBM per device.

```python
import jax
import jax.numpy as jnp
from jax import lax

BATCH = 1
CHUNK_LEN = 4096
D_MODEL = 4096
D_RNN = 4096
FF_DIM = 12288
NUM_HEADS = 16
HEAD_DIM = 256
WINDOW = 2048
QUERY_BLOCK = 64
BLOCK_W = D_RNN // NUM_HEADS
ROT_DIM = HEAD_DIM // 2


def draw_normal(key_in, arr_shape, scale_by):
    return (jax.random.normal(key_in, arr_shape, jnp.float32) * scale_by).astype(jnp.bfloat16)


def setup_inputs(seed: int = 0, part: int = 0) -> dict:
    part_keys = jax.random.split(jax.random.fold_in(jax.random.key(seed), part), 5)
    weight_keys = jax.random.split(jax.random.key(seed + 1), 17)
    lam_target = 10.0 ** jax.random.uniform(weight_keys[16], (2, D_RNN), jnp.float32, -6.0, -3.0)
    return {
        'hidden_in': draw_normal(part_keys[0], (BATCH, CHUNK_LEN, D_MODEL), 1.0),
        'start_pos': jax.random.randint(part_keys[1], (BATCH,), WINDOW, 8 * WINDOW, jnp.int32),
        'h_init': jax.random.normal(part_keys[2], (BATCH, 2, D_RNN), jnp.float32),
        'k_cache': draw_normal(part_keys[3], (BATCH, WINDOW, HEAD_DIM), 1.0),
        'v_cache': draw_normal(part_keys[4], (BATCH, WINDOW, HEAD_DIM), 1.0),
        'w_x': draw_normal(weight_keys[0], (2, D_MODEL, D_RNN), D_MODEL ** -0.5),
        'w_y': draw_normal(weight_keys[1], (2, D_MODEL, D_RNN), D_MODEL ** -0.5),
        'conv_w': draw_normal(weight_keys[2], (2, 4, D_RNN), 0.5),
        'conv_b': draw_normal(weight_keys[3], (2, D_RNN), 0.5),
        'gate_wi': draw_normal(weight_keys[4], (2, NUM_HEADS, BLOCK_W, BLOCK_W), BLOCK_W ** -0.5),
        'gate_wa': draw_normal(weight_keys[5], (2, NUM_HEADS, BLOCK_W, BLOCK_W), BLOCK_W ** -0.5),
        'gate_bi': draw_normal(weight_keys[6], (2, D_RNN), 1.0),
        'gate_ba': draw_normal(weight_keys[7], (2, D_RNN), 1.0),
        'lru_lambda': jnp.log(jnp.expm1(lam_target)),
        'w_rnn_out': draw_normal(weight_keys[8], (2, D_RNN, D_MODEL), D_RNN ** -0.5),
        'w_q': draw_normal(weight_keys[9], (D_MODEL, NUM_HEADS * HEAD_DIM), 3.0 * D_MODEL ** -0.5),
        'w_k': draw_normal(weight_keys[10], (D_MODEL, HEAD_DIM), D_MODEL ** -0.5),
        'w_v': draw_normal(weight_keys[11], (D_MODEL, HEAD_DIM), D_MODEL ** -0.5),
        'w_attn_out': draw_normal(weight_keys[12], (NUM_HEADS * HEAD_DIM, D_MODEL), 2.0 * (NUM_HEADS * HEAD_DIM) ** -0.5),
        'w_gate': draw_normal(weight_keys[13], (3, D_MODEL, FF_DIM), D_MODEL ** -0.5),
        'w_up': draw_normal(weight_keys[14], (3, D_MODEL, FF_DIM), D_MODEL ** -0.5),
        'w_down': draw_normal(weight_keys[15], (3, FF_DIM, D_MODEL), FF_DIM ** -0.5),
    }


def rms_norm(values):
    as_f32 = values.astype(jnp.float32)
    inv_rms = lax.rsqrt(jnp.mean(as_f32 * as_f32, axis=-1, keepdims=True) + 1e-6)
    return (as_f32 * inv_rms).astype(jnp.bfloat16)


def apply_rope(values, positions):
    half_dim = ROT_DIM // 2
    inv_freq = 10000.0 ** (-2.0 * jnp.arange(half_dim, dtype=jnp.float32) / ROT_DIM)
    angles = positions[:, :, None, None] * inv_freq
    cos_a = jnp.cos(angles)
    sin_a = jnp.sin(angles)
    first_half = values[..., :half_dim]
    second_half = values[..., half_dim:ROT_DIM]
    return jnp.concatenate([first_half * cos_a - second_half * sin_a, second_half * cos_a + first_half * sin_a, values[..., ROT_DIM:]], axis=-1)


def order_cache(cache_in, offset):
    doubled = jnp.concatenate([cache_in, cache_in], axis=0)
    return lax.dynamic_slice_in_dim(doubled, offset, WINDOW, axis=0)


def place_cache(ordered, shift_by):
    doubled = jnp.concatenate([ordered, ordered], axis=0)
    return lax.dynamic_slice_in_dim(doubled, (WINDOW - shift_by) % WINDOW, WINDOW, axis=0)


def recurrent_layer(residual, h_start, w_x, w_y, conv_w, conv_b, gate_wi, gate_wa, gate_bi, gate_ba, lru_lambda, w_rnn_out):
    normed = rms_norm(residual)
    y_branch = jax.nn.gelu(jnp.dot(normed, w_y, preferred_element_type=jnp.float32)).astype(jnp.bfloat16)
    u_branch = jnp.dot(normed, w_x, preferred_element_type=jnp.float32).astype(jnp.bfloat16)
    padded = jnp.pad(u_branch, ((0, 0), (3, 0), (0, 0))).astype(jnp.float32)
    conv_acc = conv_b.astype(jnp.float32) + padded[:, 0:CHUNK_LEN] * conv_w[0].astype(jnp.float32)
    for tap_idx in range(1, 4):
        conv_acc = conv_acc + padded[:, tap_idx:tap_idx + CHUNK_LEN] * conv_w[tap_idx].astype(jnp.float32)
    conv_out = conv_acc.astype(jnp.bfloat16)
    blocks = conv_out.reshape(BATCH, CHUNK_LEN, NUM_HEADS, BLOCK_W).astype(jnp.float32)
    gate_in = jax.nn.sigmoid(jnp.einsum('bthi,hij->bthj', blocks, gate_wi.astype(jnp.float32)).reshape(BATCH, CHUNK_LEN, D_RNN) + gate_bi.astype(jnp.float32))
    gate_a = jax.nn.sigmoid(jnp.einsum('bthi,hij->bthj', blocks, gate_wa.astype(jnp.float32)).reshape(BATCH, CHUNK_LEN, D_RNN) + gate_ba.astype(jnp.float32))
    log_a = -8.0 * gate_a * jax.nn.softplus(lru_lambda)
    lru_drive = conv_out.astype(jnp.float32) * gate_in * jnp.sqrt(-jnp.expm1(2.0 * log_a))

    def scan_step(h_state, step_in):
        decay_t, drive_t = step_in
        h_state = decay_t * h_state + drive_t
        return h_state, h_state

    h_last, h_steps = lax.scan(scan_step, h_start, (jnp.exp(log_a).swapaxes(0, 1), lru_drive.swapaxes(0, 1)))
    mixed_out = (h_steps.swapaxes(0, 1) * y_branch.astype(jnp.float32)).astype(jnp.bfloat16)
    out_f32 = jnp.dot(mixed_out, w_rnn_out, preferred_element_type=jnp.float32)
    return (residual.astype(jnp.float32) + out_f32).astype(jnp.bfloat16), h_last, u_branch[:, CHUNK_LEN - 3:]


def mlp_layer(residual, w_gate, w_up, w_down):
    normed = rms_norm(residual)
    hidden_ff = (jax.nn.gelu(jnp.dot(normed, w_gate, preferred_element_type=jnp.float32)) * jnp.dot(normed, w_up, preferred_element_type=jnp.float32)).astype(jnp.bfloat16)
    out_f32 = jnp.dot(hidden_ff, w_down, preferred_element_type=jnp.float32)
    return (residual.astype(jnp.float32) + out_f32).astype(jnp.bfloat16)


def attention_layer(residual, start_pos, k_cache, v_cache, w_q, w_k, w_v, w_attn_out):
    normed = rms_norm(residual)
    positions = (start_pos[:, None] + jnp.arange(CHUNK_LEN)[None, :]).astype(jnp.float32)
    queries = jnp.dot(normed, w_q, preferred_element_type=jnp.float32).reshape(BATCH, CHUNK_LEN, NUM_HEADS, HEAD_DIM)
    queries = (apply_rope(queries, positions) * HEAD_DIM ** -0.5).astype(jnp.bfloat16)
    keys_new = apply_rope(jnp.dot(normed, w_k, preferred_element_type=jnp.float32)[:, :, None, :], positions)[:, :, 0].astype(jnp.bfloat16)
    values_new = jnp.dot(normed, w_v, preferred_element_type=jnp.float32).astype(jnp.bfloat16)
    old_offset = start_pos % WINDOW
    keys_all = jnp.concatenate([jax.vmap(order_cache)(k_cache, old_offset), keys_new], axis=1)
    values_all = jnp.concatenate([jax.vmap(order_cache)(v_cache, old_offset), values_new], axis=1)
    num_blocks = CHUNK_LEN // QUERY_BLOCK
    query_blocks = queries.reshape(BATCH, num_blocks, QUERY_BLOCK, NUM_HEADS, HEAD_DIM).swapaxes(0, 1)
    row_ids = jnp.arange(QUERY_BLOCK)[:, None]
    col_ids = jnp.arange(WINDOW + QUERY_BLOCK)[None, :]
    allowed = (col_ids > row_ids) & (col_ids <= row_ids + WINDOW)

    def one_block(block_in):
        query_blk, block_idx = block_in
        key_blk = lax.dynamic_slice_in_dim(keys_all, block_idx * QUERY_BLOCK, WINDOW + QUERY_BLOCK, axis=1).astype(jnp.float32)
        value_blk = lax.dynamic_slice_in_dim(values_all, block_idx * QUERY_BLOCK, WINDOW + QUERY_BLOCK, axis=1).astype(jnp.float32)
        scores = jnp.einsum('bqhd,bkd->bhqk', query_blk.astype(jnp.float32), key_blk)
        scores = jnp.where(allowed, scores, -1e30)
        attn_probs = jax.nn.softmax(scores, axis=-1).astype(jnp.bfloat16).astype(jnp.float32)
        return jnp.einsum('bhqk,bkd->bqhd', attn_probs, value_blk).astype(jnp.bfloat16)

    attended = lax.map(one_block, (query_blocks, jnp.arange(num_blocks)))
    attended = attended.swapaxes(0, 1).reshape(BATCH, CHUNK_LEN, NUM_HEADS * HEAD_DIM)
    out_f32 = jnp.dot(attended, w_attn_out, preferred_element_type=jnp.float32)
    new_shift = (start_pos + CHUNK_LEN) % WINDOW
    k_final = jax.vmap(place_cache)(keys_all[:, CHUNK_LEN:], new_shift)
    v_final = jax.vmap(place_cache)(values_all[:, CHUNK_LEN:], new_shift)
    return (residual.astype(jnp.float32) + out_f32).astype(jnp.bfloat16), k_final, v_final


def reference(hidden_in, start_pos, h_init, k_cache, v_cache, w_x, w_y, conv_w, conv_b, gate_wi, gate_wa, gate_bi, gate_ba, lru_lambda, w_rnn_out, w_q, w_k, w_v, w_attn_out, w_gate, w_up, w_down):
    residual = hidden_in
    h_list = []
    conv_list = []
    for layer_idx in range(2):
        residual, h_last, conv_last = recurrent_layer(residual, h_init[:, layer_idx], w_x[layer_idx], w_y[layer_idx], conv_w[layer_idx], conv_b[layer_idx], gate_wi[layer_idx], gate_wa[layer_idx], gate_bi[layer_idx], gate_ba[layer_idx], lru_lambda[layer_idx], w_rnn_out[layer_idx])
        h_list.append(h_last)
        conv_list.append(conv_last)
        residual = mlp_layer(residual, w_gate[layer_idx], w_up[layer_idx], w_down[layer_idx])
    residual, k_final, v_final = attention_layer(residual, start_pos, k_cache, v_cache, w_q, w_k, w_v, w_attn_out)
    residual = mlp_layer(residual, w_gate[2], w_up[2], w_down[2])
    return (residual, jnp.stack(h_list, axis=1), jnp.stack(conv_list, axis=1), k_final, v_final)
```

```python
import functools

import jax
import jax.numpy as jnp
from jax import lax
from jax.experimental import pallas as pl
from jax.experimental.pallas import tpu as pltpu
from jax.sharding import PartitionSpec as P

ROPE_BASE = 10000.0
NORM_EPS = 1e-6
BF16 = jnp.bfloat16
F32 = jnp.float32
ARG_SPECS = (P('dp', 'sp', None), P('dp'), P('dp', None, 'tp'), P('dp', None, None), P('dp', None, None), P(None, None, 'tp'), P(None, None, 'tp'), P(None, None, 'tp'), P(None, 'tp'), P(None, 'tp', None, None), P(None, 'tp', None, None), P(None, 'tp'), P(None, 'tp'), P(None, 'tp'), P(None, 'tp', None), P(None, 'tp'), P(None, None), P(None, None), P('tp', None), P(None, None, 'tp'), P(None, None, 'tp'), P(None, 'tp', None))
OUT_SPECS = (P('dp', 'sp', None), P('dp', None, 'tp'), P('dp', None, None, 'tp'), P('dp', None, None), P('dp', None, None))

HALO = 16
SEGS = 8
LANES = 128
SWAP = [(0, 1), (1, 0)]


def dot(a, b):
    return jnp.dot(a, b, preferred_element_type=F32)


def swap(a):
    return lax.ppermute(a, 'tp', SWAP)


def rms_norm(values):
    as_f32 = values.astype(F32)
    inv_rms = lax.rsqrt(jnp.mean(as_f32 * as_f32, axis=-1, keepdims=True) + NORM_EPS)
    return (as_f32 * inv_rms).astype(BF16)


def neg_expm1(x, exp_x):
    p = 1.0 / 5040.0
    for c in (1.0 / 720.0, 1.0 / 120.0, 1.0 / 24.0, 1.0 / 6.0, 0.5, 1.0):
        p = p * x + c
    return jnp.where(x > -0.3, -x * p, 1.0 - exp_x)


def rec_pre_kernel(n_ref, wx_ref, wy_ref, cw_ref, cb_ref, wi_ref, wa_ref, bi_ref, ba_ref, sp_ref,
                   y_ref, h_ref, a_ref, end_ref, tail_ref, ubuf, abuf, bbuf):
    rows = n_ref.shape[0] - HALO
    seg = rows // SEGS
    y = jnp.dot(n_ref[HALO:, :], wy_ref[...], preferred_element_type=F32)
    y_ref[...] = jax.nn.gelu(y).astype(BF16)
    u = jnp.dot(n_ref[...], wx_ref[...], preferred_element_type=F32).astype(BF16)
    tail_ref[...] = u[rows + HALO - 8:, :].astype(F32)
    ubuf[...] = u.astype(F32)
    v = cb_ref[...].astype(F32)
    for k in range(4):
        v = v + ubuf[pl.ds(HALO - 3 + k, rows), :] * cw_ref[k:k + 1, :].astype(F32)
    v = v.astype(BF16)
    gi = jax.nn.sigmoid(jnp.dot(v, wi_ref[0], preferred_element_type=F32) + bi_ref[...].astype(F32))
    ga = jax.nn.sigmoid(jnp.dot(v, wa_ref[0], preferred_element_type=F32) + ba_ref[...].astype(F32))
    log_a = ga * sp_ref[...]
    a = jnp.exp(log_a)
    drive = v.astype(F32) * gi * jnp.sqrt(neg_expm1(2.0 * log_a, a * a))
    lanes = h_ref.shape[2]
    parts = h_ref.shape[0]
    for p in range(parts):
        abuf[p] = a[:, p * lanes:(p + 1) * lanes]
        bbuf[p] = drive[:, p * lanes:(p + 1) * lanes]

    def step(i, c):
        rows_i = pl.ds(i, SEGS, stride=seg)
        out = []
        for p in range(parts):
            h, acc = c[p]
            at = abuf[p, rows_i, :]
            h = at * h + bbuf[p, rows_i, :]
            acc = acc * at
            h_ref[p, rows_i, :] = h
            a_ref[p, rows_i, :] = acc
            out.append((h, acc))
        return tuple(out)

    zero = jnp.zeros((SEGS, lanes), F32)
    ends = lax.fori_loop(0, seg, step, tuple((zero, zero + 1.0) for _ in range(parts)), unroll=8)
    for p in range(parts):
        cols = slice(p * lanes, (p + 1) * lanes)
        end_ref[0:SEGS, cols] = ends[p][0]
        end_ref[SEGS:2 * SEGS, cols] = ends[p][1]


def rec_pre(n_ext, w_x, w_y, conv_w, conv_b, gate_wi, gate_wa, gate_bi, gate_ba, lru_lambda):
    rows = n_ext.shape[0] - HALO
    width = w_x.shape[1]
    blk = gate_wi.shape[1]
    nb = width // blk
    sp8 = -8.0 * jax.nn.softplus(lru_lambda)
    row = lambda j: (0, j)
    vec = pl.BlockSpec((1, blk), row)
    return pl.pallas_call(
        rec_pre_kernel,
        grid=(nb,),
        in_specs=[
            pl.BlockSpec((rows + HALO, n_ext.shape[1]), lambda j: (0, 0), pipeline_mode=pl.Buffered(1)),
            pl.BlockSpec((w_x.shape[0], blk), row),
            pl.BlockSpec((w_y.shape[0], blk), row),
            pl.BlockSpec((4, blk), row),
            vec,
            pl.BlockSpec((1, blk, blk), lambda j: (j, 0, 0)),
            pl.BlockSpec((1, blk, blk), lambda j: (j, 0, 0)),
            vec, vec, vec,
        ],
        out_specs=[
            pl.BlockSpec((rows, blk), row),
            pl.BlockSpec((blk // LANES, rows, LANES), lambda j: (j, 0, 0)),
            pl.BlockSpec((blk // LANES, rows, LANES), lambda j: (j, 0, 0)),
            pl.BlockSpec((2 * SEGS, blk), row),
            pl.BlockSpec((8, blk), row),
        ],
        out_shape=[
            jax.ShapeDtypeStruct((rows, width), BF16),
            jax.ShapeDtypeStruct((width // LANES, rows, LANES), F32),
            jax.ShapeDtypeStruct((width // LANES, rows, LANES), F32),
            jax.ShapeDtypeStruct((2 * SEGS, width), F32),
            jax.ShapeDtypeStruct((8, width), F32),
        ],
        scratch_shapes=[
            pltpu.VMEM((rows + HALO, blk), F32),
            pltpu.VMEM((blk // LANES, rows, LANES), F32),
            pltpu.VMEM((blk // LANES, rows, LANES), F32),
        ],
        compiler_params=pltpu.CompilerParams(vmem_limit_bytes=60 * 1024 * 1024),
        cost_estimate=pl.CostEstimate(flops=4 * rows * n_ext.shape[1] * width, bytes_accessed=60_000_000, transcendentals=0),
        name='rec_pre',
    )(n_ext, w_x, w_y, conv_w, conv_b[None], gate_wi, gate_wa, gate_bi[None], gate_ba[None], sp8[None])


def rec_mix_kernel(h_ref, a_ref, c_ref, y_ref, o_ref):
    segs = c_ref.shape[0]
    seg = h_ref.shape[1] // segs
    for s in range(segs):
        rows = slice(s * seg, (s + 1) * seg)
        h = h_ref[0, rows, :] + a_ref[0, rows, :] * c_ref[s:s + 1, :]
        o_ref[rows, :] = (h * y_ref[rows, :].astype(F32)).astype(BF16)


def rec_mix(h_seg, a_seg, carries, y, lo, hi):
    rows, width = y.shape
    toks = hi - lo
    segs = SEGS * toks // rows
    b = lo // toks
    return pl.pallas_call(
        rec_mix_kernel,
        grid=(width // LANES,),
        in_specs=[
            pl.BlockSpec((1, toks, LANES), lambda j: (j, b, 0)),
            pl.BlockSpec((1, toks, LANES), lambda j: (j, b, 0)),
            pl.BlockSpec((segs, LANES), lambda j: (0, j)),
            pl.BlockSpec((toks, LANES), lambda j: (b, j)),
        ],
        out_specs=pl.BlockSpec((toks, LANES), lambda j: (0, j)),
        out_shape=jax.ShapeDtypeStruct((toks, width), BF16),
        cost_estimate=pl.CostEstimate(flops=4_000_000_000, bytes_accessed=12 * toks * width, transcendentals=0),
        name='rec_mix',
    )(h_seg, a_seg, carries[lo * SEGS // rows:hi * SEGS // rows], y)


def attn_kernel(qb, window, q_ref, k_ref, v_ref, o_ref):
    j = pl.program_id(1)
    span = window + qb
    start = pl.multiple_of(j * qb, qb)
    keys = k_ref[pl.ds(start, span), :]
    vals = v_ref[pl.ds(start, span), :]
    s = lax.dot_general(q_ref[...], keys, (((1,), (1,)), ((), ())), preferred_element_type=F32)
    r = lax.broadcasted_iota(jnp.int32, (qb, qb), 0)
    c = lax.broadcasted_iota(jnp.int32, (qb, qb), 1)
    s = jnp.concatenate([jnp.where(c > r, s[:, :qb], -1e30), s[:, qb:window], jnp.where(c <= r, s[:, window:], -1e30)], axis=1)
    m = jnp.max(s, axis=1, keepdims=True)
    e = jnp.exp(s - m)
    p = (e * (1.0 / jnp.sum(e, axis=1, keepdims=True))).astype(BF16)
    o_ref[...] = jnp.dot(p, vals, preferred_element_type=F32).astype(BF16)


def attend(q, keys, vals, head_dim, window, qb=256):
    toks, width = q.shape
    heads = width // head_dim
    return pl.pallas_call(
        functools.partial(attn_kernel, qb, window),
        grid=(heads, toks // qb),
        in_specs=[
            pl.BlockSpec((qb, head_dim), lambda h, j: (j, h)),
            pl.BlockSpec(keys.shape, lambda h, j: (0, 0), pipeline_mode=pl.Buffered(1)),
            pl.BlockSpec(vals.shape, lambda h, j: (0, 0), pipeline_mode=pl.Buffered(1)),
        ],
        out_specs=pl.BlockSpec((qb, head_dim), lambda h, j: (j, h)),
        out_shape=jax.ShapeDtypeStruct((toks, width), BF16),
        compiler_params=pltpu.CompilerParams(vmem_limit_bytes=60 * 1024 * 1024),
        cost_estimate=pl.CostEstimate(flops=4 * toks * width * (window + qb), bytes_accessed=12_000_000, transcendentals=toks * heads * window),
        name='attend',
    )(q, keys, vals)


def apply_rope(values, cos_a, sin_a):
    half_dim = cos_a.shape[-1]
    first_half = values[..., :half_dim]
    second_half = values[..., half_dim:2 * half_dim]
    return jnp.concatenate([first_half * cos_a - second_half * sin_a, second_half * cos_a + first_half * sin_a, values[..., 2 * half_dim:]], axis=-1)


def fetch_rows(w_mine, rank, sp_size):
    part = w_mine.shape[0] // sp_size
    quarter = lax.dynamic_slice_in_dim(w_mine, rank * part, part, axis=0)
    return lax.all_gather(swap(quarter), 'sp', axis=0, tiled=True)


def project(x, mine, w_mine, w_other, groups):
    outs = []
    others = [swap(m) for m in mine]
    for (lo, hi), m, other in zip(groups, mine, others):
        p_mine = dot(m, w_mine)
        p_other = dot(other, w_other)
        outs.append((x[lo:hi].astype(F32) + (p_mine + p_other)).astype(BF16))
    return outs


def mlp(x, side, w_gate, w_up, w_down):
    half = x.shape[0] // 2
    normed = rms_norm(x)
    hidden_ff = (jax.nn.gelu(dot(normed, w_gate)) * dot(normed, w_up)).astype(BF16)
    theirs = dot(lax.dynamic_slice_in_dim(hidden_ff, (1 - side) * half, half, axis=0), w_down)
    got = swap(theirs)
    ours = dot(lax.dynamic_slice_in_dim(hidden_ff, side * half, half, axis=0), w_down)
    x_ours = lax.dynamic_slice_in_dim(x, side * half, half, axis=0)
    new = (x_ours.astype(F32) + (ours + got)).astype(BF16)
    new_other = swap(new)
    return jnp.where(side == 0, jnp.concatenate([new, new_other], axis=0), jnp.concatenate([new_other, new], axis=0))


def solution(mesh):
    sp_size = mesh.shape['sp']

    def device_fn(hidden_in, start_pos, h_init, k_cache, v_cache, w_x, w_y, conv_w, conv_b, gate_wi, gate_wa, gate_bi, gate_ba, lru_lambda, w_rnn_out, w_q, w_k, w_v, w_attn_out, w_gate, w_up, w_down):
        rank = lax.axis_index('sp')
        side = lax.axis_index('tp')
        toks = hidden_in.shape[1]
        window, head_dim = k_cache.shape[1:]
        groups = [(0, toks // 2), (toks // 2, toks)]
        x = hidden_in[0]
        rnn_other = [fetch_rows(w_rnn_out[i], rank, sp_size) for i in range(2)]
        attn_other = fetch_rows(w_attn_out, rank, sp_size)
        h_list = []
        conv_list = []
        for i in range(2):
            halo = lax.ppermute(x[toks - HALO:], 'sp', [(r, r + 1) for r in range(sp_size - 1)])
            n_ext = rms_norm(jnp.concatenate([halo, x], axis=0))
            y, h_seg, a_seg, ends, tail = rec_pre(n_ext, w_x[i], w_y[i], conv_w[i], conv_b[i], gate_wi[i], gate_wa[i], gate_bi[i], gate_ba[i], lru_lambda[i])
            h_end, a_end = ends[:SEGS], ends[SEGS:]
            h_tot, a_tot = h_end[0], a_end[0]
            for s in range(1, SEGS):
                h_tot = a_end[s] * h_tot + h_end[s]
                a_tot = a_tot * a_end[s]
            everyone = lax.all_gather(jnp.concatenate([h_tot[None], a_tot[None], tail[5:8]], axis=0), 'sp')
            carry = h_init[0, i]
            state = carry
            for r in range(sp_size):
                state = jnp.where(rank == r, carry, state)
                carry = everyone[r, 1] * carry + everyone[r, 0]
            h_list.append(carry)
            conv_list.append(everyone[sp_size - 1, 2:5].astype(BF16))
            carries = [state]
            for s in range(SEGS - 1):
                carries.append(a_end[s] * carries[-1] + h_end[s])
            carries = jnp.stack(carries)
            mixed = [rec_mix(h_seg, a_seg, carries, y, lo, hi) for lo, hi in groups]
            xs = project(x, mixed, w_rnn_out[i], rnn_other[i], groups)
            x = jnp.concatenate([mlp(xg, side, w_gate[i], w_up[i], w_down[i]) for xg in xs], axis=0)
        normed = rms_norm(x)
        half_dim = head_dim // 4
        inv_freq = ROPE_BASE ** (-2.0 * jnp.arange(half_dim, dtype=F32) / (2 * half_dim))
        positions = (start_pos[0] + rank * toks + jnp.arange(toks)).astype(F32)
        angles = positions[:, None] * inv_freq
        cos_a, sin_a = jnp.cos(angles), jnp.sin(angles)
        keys_mine = apply_rope(dot(normed, w_k), cos_a, sin_a).astype(BF16)
        vals_mine = dot(normed, w_v).astype(BF16)
        keys_chunk = lax.all_gather(keys_mine, 'sp', axis=0, tiled=True)
        vals_chunk = lax.all_gather(vals_mine, 'sp', axis=0, tiled=True)
        heads = w_q.shape[1] // head_dim
        q = dot(normed, w_q).reshape(toks, heads, head_dim)
        q = (apply_rope(q, cos_a[:, None], sin_a[:, None]) * head_dim ** -0.5).astype(BF16).reshape(toks, heads * head_dim)
        chunk_len = keys_chunk.shape[0]
        offset = start_pos[0] % window
        new_shift = (start_pos[0] + chunk_len) % window

        def order(cache):
            return lax.dynamic_slice_in_dim(jnp.concatenate([cache, cache], axis=0), offset, window, axis=0)

        def place(last):
            return lax.dynamic_slice_in_dim(jnp.concatenate([last, last], axis=0), (window - new_shift) % window, window, axis=0)

        def windowed(cache, chunk):
            both = jnp.concatenate([order(cache), chunk], axis=0)
            return lax.dynamic_slice_in_dim(both, rank * toks, window + toks, axis=0)

        att = attend(q, windowed(k_cache[0], keys_chunk), windowed(v_cache[0], vals_chunk), head_dim, window)
        xs = project(x, [att[lo:hi] for lo, hi in groups], w_attn_out, attn_other, groups)
        x = jnp.concatenate([mlp(xg, side, w_gate[2], w_up[2], w_down[2]) for xg in xs], axis=0)
        k_final = place(keys_chunk[chunk_len - window:])
        v_final = place(vals_chunk[chunk_len - window:])
        return (x[None], jnp.stack(h_list)[None], jnp.stack(conv_list)[None], k_final[None], v_final[None])

    return jax.shard_map(device_fn, mesh=mesh, in_specs=ARG_SPECS, out_specs=OUT_SPECS, check_vma=False)
```
